32 devices in a mesh: groups: 2 (over x), ctx: 16 (over z, y, core).
Axes of the slice: x: 2, y: 2, z: 4, core: 2. Of those that a mesh axis runs over, the one named last changes fastest.
Arguments:
- hidden_in: bfloat16 [4096, 2048], P(('groups', 'ctx')), parts along dimension 0, may hold values from -6 to 6
- span_order: int32 [32, 2], P('groups'), parts along dimension 0, may hold values from 0 to 31, as said below
- norm_gain: float32 [2048], replicated, may hold values from 0.5 to 1.5
- w_query: bfloat16 [2048, 2048], replicated, may hold values from -0.125 to 0.125
- w_key: bfloat16 [2048, 256], replicated, may hold values from -0.125 to 0.125
- w_value: bfloat16 [2048, 256], replicated, may hold values from -0.125 to 0.125
- query_gain: float32 [128], replicated, may hold values from 1.5 to 7
- key_gain: float32 [128], replicated, may hold values from 1.5 to 7
Outputs:
- attended: bfloat16 [4096, 2048], P(('groups', 'ctx')), parts along dimension 0
The draws below stay inside these ranges and needn't reach their ends.
There are 2 independent parts, one for each index of `groups`. The reference program is written for one: setup_inputs(seed, part) draws one part's arguments, and reference() takes and returns one part's arrays. A program takes and returns all parts, laid end to end along the dimension named above; an argument that names none is the same for every part. Nothing has to cross between parts.
Inputs may be any that keep to these rules, and one draw needn't show every extreme that they name: `span_order`: row d holds a span c and the span 2 * 16 - 1 - c with c < 16; the rows together name every span once; a device's first 64 rows are its column 0 span.
All inputs are finite; a program needn't handle non-finite values.
Results may differ from the reference program's by a relative error of at most 0.0075.
The reference program's roundings to bfloat16 on the way count: a program that leaves them out, or rounds other values in their place, can miss the bound.
Values may be sent and summed in bfloat16 or wider, within the bound.
A program may use at most 128 MiB of HBM per device.

```python
import math
import jax
import jax.numpy as jnp
from jax import lax

D = 2048
HEADS = 16
KV_HEADS = 2
HEAD = 128
TOKENS = 2048
N_CTX = 16


def draw_span_order(key, part):
    shuffled = jax.random.permutation(jax.random.fold_in(key, 11), N_CTX).astype(jnp.int32)
    return jnp.stack([shuffled, 2 * N_CTX - 1 - shuffled], axis=1)


def draw_query_gain(key, part):
    subkey = jax.random.fold_in(key, 23)
    return jax.random.uniform(subkey, (HEAD,), jnp.float32, 1.5, 3.0)


def draw_key_gain(key, part):
    subkey = jax.random.fold_in(key, 37)
    return jax.random.uniform(subkey, (HEAD,), jnp.float32, 1.5, 3.0)


def block_levels(stream_key, extent, split, least, top_value):
    def one(dim, parts):
        steps = jax.random.uniform(jax.random.fold_in(jax.random.fold_in(stream_key, 6), dim), (parts,), jnp.float32, least / len(split), top_value / len(split))
        return jnp.repeat(jnp.exp(steps), extent[dim] // parts).reshape((-1,) + (1,) * (len(extent) - dim - 1))

    loudness = one(*split[0])
    for cut in split[1:]:
        loudness = loudness * one(*cut)
    return loudness


def noise(rng, shape, deviation, limit, cuts=(), held_as=jnp.bfloat16):
    array = deviation * jax.random.normal(rng, shape, jnp.float32)
    if cuts:
        array = array * block_levels(rng, shape, cuts, -0.22, 0.18)
    return jnp.clip(array, -limit, limit).astype(held_as)


def setup_inputs(seed: int = 0, part: int = 0) -> dict:
    key_of = jax.random.split(jax.random.key(seed), 9)
    part_keys = jax.random.split(jax.random.fold_in(key_of[8], part), 9)
    return {
        "hidden_in": noise(part_keys[0], (TOKENS, D), 1.0, 6.0, ((0, 16),)),
        "span_order": draw_span_order(jax.random.fold_in(jax.random.fold_in(key_of[8], part), 71), part),
        "norm_gain": jnp.clip(1.0 + 0.1 * jax.random.normal(key_of[2], (D,), jnp.float32), 0.5, 1.5),
        "w_query": noise(key_of[3], (D, HEADS * HEAD), D ** -0.5, 0.125),
        "w_key": noise(key_of[4], (D, KV_HEADS * HEAD), D ** -0.5, 0.125),
        "w_value": noise(key_of[5], (D, KV_HEADS * HEAD), D ** -0.5, 0.125),
        "query_gain": draw_query_gain(jax.random.fold_in(key_of[8], 71), part),
        "key_gain": draw_key_gain(jax.random.fold_in(key_of[8], 71), part),
    }


EPSILON = 1e-06
THETA = 1000000.0

def scaled(entries, gains):
    mean_square = lax.optimization_barrier(jnp.mean(entries * entries, axis=-1, keepdims=True))
    return entries * lax.rsqrt(mean_square + EPSILON) * gains

def rotated(entries, position):
    head_width = entries.shape[-1]
    halfway = head_width // 2
    exponent = jnp.arange(halfway, dtype=jnp.float32) * (2.0 / head_width)
    inverse = jnp.power(jnp.float32(THETA), -exponent)
    angles = position.astype(jnp.float32)[:, None] * inverse[None, :]
    cosine = jnp.cos(angles)[:, None, :]
    sine_part = jnp.sin(angles)[:, None, :]
    first_half = entries[..., :halfway]
    second = entries[..., halfway:]
    return jnp.concatenate([first_half * cosine - second * sine_part, second * cosine + first_half * sine_part], axis=-1)

def project(hidden_in, norm_gain, w_query, w_key, w_value, query_gain, key_gain, position):
    row_count = hidden_in.shape[0]
    normed = scaled(hidden_in.astype(jnp.float32), norm_gain).astype(jnp.bfloat16)
    queries = jnp.dot(normed, w_query, preferred_element_type=jnp.float32).reshape(row_count, HEADS, HEAD)
    queries = rotated(scaled(queries, query_gain), position).astype(jnp.bfloat16)
    key_heads = jnp.dot(normed, w_key, preferred_element_type=jnp.float32).reshape(row_count, KV_HEADS, HEAD)
    key_heads = rotated(scaled(key_heads, key_gain), position).astype(jnp.bfloat16)
    values = jnp.dot(normed, w_value, preferred_element_type=jnp.float32).astype(jnp.bfloat16)
    return (queries, key_heads, values)

def reference(hidden_in, span_order, norm_gain, w_query, w_key, w_value, query_gain, key_gain):
    row_count = hidden_in.shape[0]
    tok_rows = row_count // N_CTX
    half_rows = tok_rows // 2
    row_index = jnp.arange(row_count, dtype=jnp.int32)
    device = row_index // tok_rows
    within = row_index % tok_rows
    span_ids = span_order[device, within // half_rows]
    position = (span_ids * half_rows + within % half_rows).astype(jnp.int32)
    queries, key_heads, values = project(hidden_in, norm_gain, w_query, w_key, w_value, query_gain, key_gain, position)
    group_size = HEADS // KV_HEADS
    block_rows = math.gcd(row_count, 256)
    keys_wide = key_heads.astype(jnp.float32)
    values_wide = values.reshape(row_count, KV_HEADS, HEAD).astype(jnp.float32)
    query_blocks = queries.reshape(row_count // block_rows, block_rows, KV_HEADS, group_size, HEAD)
    position_blocks = position.reshape(row_count // block_rows, block_rows)

    def attend(inputs):
        q_block, p_block = inputs
        scores = jnp.einsum('bcgd,kcd->cgbk', q_block.astype(jnp.float32), keys_wide) * HEAD ** (-0.5)
        visible = position[None, :] <= p_block[:, None]
        scores = jnp.where(visible, scores, -1e+30)
        row_peak = lax.optimization_barrier(jnp.max(scores, axis=-1, keepdims=True))
        weight = jnp.where(visible, jnp.exp(scores - row_peak), 0.0)
        row_total = lax.optimization_barrier(jnp.sum(weight, axis=-1))
        rounded = lax.optimization_barrier(weight.astype(jnp.bfloat16)).astype(jnp.float32)
        blended = jnp.einsum('cgbk,kcd->cgbd', rounded, values_wide) / row_total[..., None]
        return jnp.transpose(blended, (2, 0, 1, 3)).reshape(block_rows, HEADS * HEAD).astype(jnp.bfloat16)
    result = lax.map(attend, (query_blocks, position_blocks))
    return result.reshape(row_count, HEADS * HEAD)
```

```python
import functools

import jax
import jax.numpy as jnp
import numpy as np
from jax import lax
from jax.experimental import pallas as pl
from jax.experimental.pallas import tpu as pltpu
from jax.sharding import PartitionSpec as P

HEAD = 128
EPSILON = 1e-06
THETA = 1000000.0
MESH = pl.DeviceIdType.MESH
LOW = -1e30
FACTOR = HEAD ** (-0.5) * 1.4426950408889634
F32 = jnp.float32
BF16 = jnp.bfloat16


def flip(index, mask):
    for bit in range(mask.bit_length()):
        if mask >> bit & 1:
            index = index + (1 << bit) * (1 - 2 * ((index // (1 << bit)) % 2))
    return index


def kernel(
    n, heads, kv_heads,
    hidden_ref, span_ref, gain_ref, wq_hbm, wk_hbm, wv_hbm, qgain_ref, kgain_ref, inverse_ref,
    out_ref,
    wq_ref, wk_ref, wv_ref, kv_ref, q_ref, s_ref, vta_ref, vtb_ref, vtc_ref, pa_ref, pb_ref,
    acc_ref, peak_ref, total_ref,
    w_sem, recv_sem, z_sem, y_sem, c_sem,
):
    rows = hidden_ref.shape[0]
    half = rows // 2
    group = heads // kv_heads
    wide = group * half
    me = lax.axis_index("ctx")
    lanes_z = n // 4
    z, y, c = me // 4, (me // 2) % 2, me % 2

    def ident(zz, yy, cc):
        return zz * 4 + yy * 2 + cc

    def place(step, k):
        return 4 * ((z // 4 + step) % (lanes_z // 4)) + flip(z % 4, k)

    y_peer = ident(z, 1 - y, c)
    c_peer = ident(z, y, 1 - c)

    chunk = 4 * HEAD
    chunks = heads * HEAD // chunk
    load_k = pltpu.make_async_copy(wk_hbm, wk_ref, w_sem.at[0])
    load_v = pltpu.make_async_copy(wv_hbm, wv_ref, w_sem.at[1])
    load_q = [
        pltpu.make_async_copy(
            wq_hbm.at[:, pl.ds(i * chunk, chunk)], wq_ref.at[i], w_sem.at[2 + i]
        )
        for i in range(chunks)
    ]
    load_k.start()
    load_v.start()
    for copy in load_q:
        copy.start()

    barrier = pltpu.get_barrier_semaphore()
    others = [(s, k) for s in range(lanes_z // 4) for k in range(4) if (s, k) != (0, 0)]
    for peer in [y_peer, c_peer] + [ident(place(s, k), y, c) for s, k in others]:
        pl.semaphore_signal(barrier, inc=1, device_id={"ctx": peer}, device_id_type=MESH)

    def send(src, target, sem):
        return pltpu.make_async_remote_copy(
            src_ref=kv_ref.at[src],
            dst_ref=kv_ref.at[src],
            send_sem=sem,
            recv_sem=recv_sem.at[src],
            device_id={"ctx": target},
            device_id_type=MESH,
        )

    def arrived(src):
        send(src, c_peer, c_sem.at[0]).wait_recv()

    hidden = hidden_ref[...].astype(F32)
    mean_square = jnp.mean(hidden * hidden, axis=-1, keepdims=True)
    normed = (hidden * lax.rsqrt(mean_square + EPSILON) * gain_ref[...]).astype(BF16)

    own_first, own_second = span_ref[me, 0], span_ref[me, 1]
    within = lax.broadcasted_iota(jnp.int32, (rows, HEAD), 0)
    position = jnp.where(
        within < half, own_first * half + within, own_second * half + within - half
    )
    angles = position.astype(F32) * inverse_ref[...]
    cosine = jnp.cos(angles)
    sine = jnp.sin(angles)
    lane = lax.broadcasted_iota(jnp.int32, (rows, HEAD), 1)
    sine = jnp.where(lane < HEAD // 2, -sine, sine)

    def finished(entries, gains):
        square = jnp.mean(entries * entries, axis=-1, keepdims=True)
        entries = entries * lax.rsqrt(square + EPSILON) * gains
        return (entries * cosine + pltpu.roll(entries, HEAD // 2, 1) * sine).astype(BF16)

    load_k.wait()
    keys = jnp.dot(normed, wk_ref[...], preferred_element_type=F32)
    for g in range(kv_heads):
        cut = slice(g * HEAD, (g + 1) * HEAD)
        kv_ref[me, 0, :, cut] = finished(keys[:, cut], kgain_ref[...])
    load_v.wait()
    kv_ref[me, 1] = jnp.dot(normed, wv_ref[...], preferred_element_type=F32).astype(BF16)

    pl.semaphore_wait(barrier, 2 + len(others))
    send(me, c_peer, c_sem.at[0]).start()
    send(me, y_peer, y_sem.at[0]).start()
    for i, (s, k) in enumerate(others):
        send(me, ident(place(s, k), y, c), z_sem.at[i]).start()

    ordered = own_first < own_second
    own_low = jnp.minimum(own_first, own_second)
    for i in range(chunks):
        load_q[i].wait()
        part = jnp.dot(normed, wq_ref[i], preferred_element_type=F32)
        for j in range(chunk // HEAD):
            head = i * (chunk // HEAD) + j
            done = finished(part[:, j * HEAD:(j + 1) * HEAD], qgain_ref[...])
            g, r = head // group, head % group
            first, second = done[:half], done[half:]
            q_ref[g, r * half:(r + 1) * half, :HEAD] = jnp.where(ordered, first, second)
            q_ref[g, r * half:(r + 1) * half, HEAD:] = jnp.where(ordered, second, first)

    def transposed_dot(a, b):
        return lax.dot_general(a, b, (((1,), (1,)), ((), ())), preferred_element_type=F32)

    def block_peak(block):
        tall = block.shape[0]
        return jnp.max(block.reshape(tall // 8, 8, wide), axis=0)

    visible = (
        lax.broadcasted_iota(jnp.int32, (half, wide), 0)
        <= lax.broadcasted_iota(jnp.int32, (half, wide), 1) % half
    )

    def score(zz, k, own, peaks):
        sources = []
        for yy, cc in ((y, c), (y, 1 - c), (1 - y, c), (1 - y, 1 - c)):
            src = ident(zz, yy, cc)
            upper = span_ref[src, 0] > span_ref[src, 1]
            early = jnp.minimum(span_ref[src, 0], span_ref[src, 1]) < own_low
            sources.append((src, upper, early))
        for g in range(kv_heads):
            cut = slice(g * HEAD, (g + 1) * HEAD)

            def piece(src, part, upper):
                first = kv_ref[src, part, :half, cut]
                second = kv_ref[src, part, half:, cut]
                return jnp.where(upper, second, first)

            span = slice(k * 4 * half, (k + 1) * 4 * half)
            low_keys = jnp.concatenate([piece(s, 0, up) for s, up, e in sources], axis=0)
            scores = transposed_dot(low_keys, q_ref[g, :, HEAD:])
            s_ref[g, 0, span, :] = scores
            peaks[g][1] = jnp.maximum(peaks[g][1], block_peak(scores))
            low_values = jnp.concatenate([piece(s, 1, up) for s, up, e in sources], axis=0)
            vta_ref[g, :, span] = low_values.T

            def parted(part):
                early_side, late_side = [], []
                for src, upper, early in sources:
                    block = piece(src, part, upper == early)
                    early_side.append(jnp.where(early, block, jnp.zeros_like(block)))
                    late_side.append(jnp.where(early, jnp.zeros_like(block), block))
                return jnp.concatenate(
                    [jnp.concatenate(early_side, axis=0), jnp.concatenate(late_side, axis=0)],
                    axis=1,
                )

            mixed = transposed_dot(parted(0), q_ref[g])
            for j, (src, upper, early) in enumerate(sources):
                scores = mixed[j * half:(j + 1) * half]
                if own and j == 0:
                    scores = jnp.where(visible, scores, LOW)
                at = (k * 4 + j) * half
                s_ref[g, 1, at:at + half, :] = scores
                peak = block_peak(scores)
                peaks[g][0] = jnp.maximum(peaks[g][0], jnp.where(early, peak, LOW))
                peaks[g][1] = jnp.maximum(peaks[g][1], jnp.where(early, LOW, peak))
            vtb_ref[g, :, span] = parted(1).T
            if own:
                src, upper, early = sources[0]
                scores = transposed_dot(piece(src, 0, upper), q_ref[g, :, :HEAD])
                scores = jnp.where(visible, scores, LOW)
                s_ref[g, 1, 16 * half:17 * half, :] = scores
                peaks[g][0] = jnp.maximum(peaks[g][0], block_peak(scores))
                vtc_ref[g] = piece(src, 1, upper).T

    def take(step, k):
        i = step * 4 + k
        src = ident(place(step, k), y, c)
        arrived(src)
        send(src, y_peer, y_sem.at[i]).start()
        send(src, c_peer, c_sem.at[2 * i]).start()

    def pass_on(step, k):
        i = step * 4 + k
        src = ident(place(step, k), 1 - y, c)
        arrived(src)
        send(src, c_peer, c_sem.at[2 * i + 1]).start()

    def last(step, k):
        arrived(ident(place(step, k), y, 1 - c))
        arrived(ident(place(step, k), 1 - y, 1 - c))

    def sums(block):
        tall = block.shape[0]
        return jnp.sum(block.reshape(tall // 8, 8, wide), axis=0)

    def absorb(step, first, peaks):
        for g in range(kv_heads):
            new = [jnp.max(peaks[g][t], axis=0, keepdims=True) for t in range(2)]
            if not first:
                new = [jnp.maximum(new[t], peak_ref[g, t]) for t in range(2)]
            totals = [jnp.zeros((8, wide), F32), jnp.zeros((8, wide), F32)]
            for k in range(4):
                at = k * 4 * half
                weight = jnp.exp2((s_ref[g, 0, at:at + 4 * half, :] - new[1]) * FACTOR)
                totals[1] = totals[1] + sums(weight)
                pa_ref[at:at + 4 * half, :] = weight.astype(BF16)
                for j, (yy, cc) in enumerate(
                    ((y, c), (y, 1 - c), (1 - y, c), (1 - y, 1 - c))
                ):
                    src = ident(place(step, k), yy, cc)
                    early = jnp.minimum(span_ref[src, 0], span_ref[src, 1]) < own_low
                    spot = at + j * half
                    peak = jnp.where(early, new[0], new[1])
                    weight = jnp.exp2((s_ref[g, 1, spot:spot + half, :] - peak) * FACTOR)
                    part = sums(weight)
                    totals[0] = totals[0] + jnp.where(early, part, 0.0)
                    totals[1] = totals[1] + jnp.where(early, 0.0, part)
                    pb_ref[spot:spot + half, :] = weight.astype(BF16)
            mixed = jnp.dot(vtb_ref[g], pb_ref[...], preferred_element_type=F32)
            added = [
                mixed[:HEAD],
                mixed[HEAD:] + jnp.dot(vta_ref[g], pa_ref[...], preferred_element_type=F32),
            ]
            if first:
                weight = jnp.exp2((s_ref[g, 1, 16 * half:17 * half, :] - new[0]) * FACTOR)
                totals[0] = totals[0] + sums(weight)
                added[0] = added[0] + jnp.dot(
                    vtc_ref[g], weight.astype(BF16), preferred_element_type=F32
                )
            for t in range(2):
                total = jnp.sum(totals[t], axis=0, keepdims=True)
                if first:
                    acc_ref[g, t] = added[t]
                    total_ref[g, t] = total
                else:
                    decay = jnp.exp2((peak_ref[g, t] - new[t]) * FACTOR)
                    acc_ref[g, t] = acc_ref[g, t] * decay + added[t]
                    total_ref[g, t] = total_ref[g, t] * decay + total
                peak_ref[g, t] = new[t]

    def nothing():
        return [[jnp.full((8, wide), LOW, F32) for t in range(2)] for g in range(kv_heads)]

    peaks = nothing()
    arrived(c_peer)
    pass_on(0, 0)
    take(0, 1)
    arrived(ident(z, 1 - y, 1 - c))
    score(z, 0, True, peaks)
    take(0, 2)
    pass_on(0, 1)
    take(0, 3)
    last(0, 1)
    score(place(0, 1), 1, False, peaks)
    pass_on(0, 2)
    last(0, 2)
    score(place(0, 2), 2, False, peaks)
    pass_on(0, 3)
    last(0, 3)
    score(place(0, 3), 3, False, peaks)
    absorb(0, True, peaks)

    def further(step, carry):
        peaks = nothing()
        for k in range(4):
            take(step, k)
        for k in range(4):
            pass_on(step, k)
        for k in range(4):
            last(step, k)
            score(place(step, k), k, False, peaks)
        absorb(step, False, peaks)
        return carry

    if lanes_z > 4:
        lax.fori_loop(1, lanes_z // 4, further, 0)

    for g in range(kv_heads):
        low = acc_ref[g, 0] / total_ref[g, 0]
        high = acc_ref[g, 1] / total_ref[g, 1]
        for r in range(0, group, 2):
            low_rows = low[:, r * half:(r + 2) * half].T
            high_rows = high[:, r * half:(r + 2) * half].T
            first = jnp.where(ordered, low_rows, high_rows).astype(BF16)
            second = jnp.where(ordered, high_rows, low_rows).astype(BF16)
            for e in range(2):
                at = (g * group + r + e) * HEAD
                out_ref[:half, at:at + HEAD] = first[e * half:(e + 1) * half]
                out_ref[half:, at:at + HEAD] = second[e * half:(e + 1) * half]

    for i in range(len(others)):
        send(me, y_peer, z_sem.at[i]).wait_send()
    for i in range(lanes_z):
        send(me, y_peer, y_sem.at[i]).wait_send()
    for i in range(2 * lanes_z):
        send(me, y_peer, c_sem.at[i]).wait_send()


def solution(mesh):
    n = mesh.shape["ctx"]

    def body(hidden_in, span_order, norm_gain, w_query, w_key, w_value, query_gain, key_gain):
        rows, depth = hidden_in.shape
        heads, kv_heads = w_query.shape[1] // HEAD, w_key.shape[1] // HEAD
        half = rows // 2
        wide = heads // kv_heads * half
        frequency = THETA ** (-np.arange(HEAD // 2, dtype=np.float64) * (2.0 / HEAD))
        inverse = jnp.asarray(np.tile(frequency, 2)[None, :], F32)
        vmem = pl.BlockSpec(memory_space=pltpu.VMEM)
        anywhere = pl.BlockSpec(memory_space=pl.ANY)
        chunk = 4 * HEAD
        chunks = heads * HEAD // chunk
        return pl.pallas_call(
            functools.partial(kernel, n, heads, kv_heads),
            out_shape=jax.ShapeDtypeStruct((rows, heads * HEAD), BF16),
            in_specs=[
                vmem, pl.BlockSpec(memory_space=pltpu.SMEM), vmem,
                anywhere, anywhere, anywhere, vmem, vmem, vmem,
            ],
            out_specs=vmem,
            scratch_shapes=[
                pltpu.VMEM((chunks, depth, chunk), BF16),
                pltpu.VMEM((depth, kv_heads * HEAD), BF16),
                pltpu.VMEM((depth, kv_heads * HEAD), BF16),
                pltpu.VMEM((n, 2, rows, kv_heads * HEAD), BF16),
                pltpu.VMEM((kv_heads, wide, 2 * HEAD), BF16),
                pltpu.VMEM((kv_heads, 2, 17 * half, wide), F32),
                pltpu.VMEM((kv_heads, HEAD, 16 * half), BF16),
                pltpu.VMEM((kv_heads, 2 * HEAD, 16 * half), BF16),
                pltpu.VMEM((kv_heads, HEAD, half), BF16),
                pltpu.VMEM((16 * half, wide), BF16),
                pltpu.VMEM((16 * half, wide), BF16),
                pltpu.VMEM((kv_heads, 2, HEAD, wide), F32),
                pltpu.VMEM((kv_heads, 2, 1, wide), F32),
                pltpu.VMEM((kv_heads, 2, 1, wide), F32),
                pltpu.SemaphoreType.DMA((2 + chunks,)),
                pltpu.SemaphoreType.DMA((n,)),
                pltpu.SemaphoreType.DMA((n // 4,)),
                pltpu.SemaphoreType.DMA((n // 4,)),
                pltpu.SemaphoreType.DMA((n // 2,)),
            ],
            compiler_params=pltpu.CompilerParams(
                collective_id=0, has_side_effects=True, vmem_limit_bytes=60 * 1024 * 1024
            ),
        )(
            hidden_in, span_order, norm_gain.reshape(1, -1), w_query, w_key, w_value,
            query_gain.reshape(1, -1), key_gain.reshape(1, -1), inverse,
        )

    in_specs = (P(("groups", "ctx"), None), P("groups", None), P(), P(), P(), P(), P(), P())
    out_specs = P(("groups", "ctx"), None)
    return jax.shard_map(body, mesh=mesh, in_specs=in_specs, out_specs=out_specs, check_vma=False)
```

```python
import functools

import jax
import jax.numpy as jnp
import numpy as np
from jax import lax
from jax.experimental import pallas as pl
from jax.experimental.pallas import tpu as pltpu
from jax.sharding import PartitionSpec as P

HEAD = 128
EPSILON = 1e-06
THETA = 1000000.0
MESH = pl.DeviceIdType.MESH
LOW = -1e30
FACTOR = HEAD ** (-0.5) * 1.4426950408889634
F32 = jnp.float32
BF16 = jnp.bfloat16


def flip(index, mask):
    for bit in range(mask.bit_length()):
        if mask >> bit & 1:
            index = index + (1 << bit) * (1 - 2 * ((index // (1 << bit)) % 2))
    return index


def kernel(
    n, heads, kv_heads,
    hidden_hbm, span_ref, gain_ref, wq_hbm, wk_hbm, wv_hbm, qgain_ref, kgain_ref, inverse_ref,
    out_ref,
    hidden_ref, wq_ref, wk_ref, wv_ref, kv_ref, q_ref, s_ref, vta_ref, vtb_ref, vtc_ref, pa_ref, pb_ref,
    acc_ref, peak_ref, total_ref,
    w_sem, recv_sem, up_sem, down_sem, y_sem, c_sem,
):
    rows = hidden_ref.shape[0]
    half = rows // 2
    group = heads // kv_heads
    wide = group * half
    me = lax.axis_index("ctx")
    lanes_z = n // 4
    z, y, c = me // 4, (me // 2) % 2, me % 2

    def ident(zz, yy, cc):
        return zz * 4 + yy * 2 + cc

    def place(step, k):
        return 4 * ((z // 4 + step) % (lanes_z // 4)) + flip(z % 4, k)

    y_peer = ident(z, 1 - y, c)
    c_peer = ident(z, y, 1 - c)

    chunk = 4 * HEAD
    chunks = heads * HEAD // chunk
    load_k = pltpu.make_async_copy(wk_hbm, wk_ref, w_sem.at[0])
    load_v = pltpu.make_async_copy(wv_hbm, wv_ref, w_sem.at[1])
    load_q = [
        pltpu.make_async_copy(
            wq_hbm.at[:, pl.ds(i * chunk, chunk)], wq_ref.at[i], w_sem.at[2 + i]
        )
        for i in range(chunks)
    ]
    load_h = pltpu.make_async_copy(hidden_hbm, hidden_ref, w_sem.at[2 + chunks])
    load_h.start()
    load_k.start()
    load_v.start()

    barrier = pltpu.get_barrier_semaphore()
    below, above = z > 0, z < lanes_z - 1

    def greet(peer):
        pl.semaphore_signal(barrier, inc=1, device_id={"ctx": peer}, device_id_type=MESH)

    greet(y_peer)
    greet(c_peer)
    pl.when(below)(lambda: greet(me - 4))
    pl.when(above)(lambda: greet(me + 4))

    def send(src, p, target, sem):
        return pltpu.make_async_remote_copy(
            src_ref=kv_ref.at[src, p],
            dst_ref=kv_ref.at[src, p],
            send_sem=sem,
            recv_sem=recv_sem.at[src, p],
            device_id={"ctx": target},
            device_id_type=MESH,
        )

    def arrived(src, p):
        send(src, p, c_peer, c_sem.at[0, p]).wait_recv()

    def to_y(zz, p):
        return send(ident(zz, y, c), p, y_peer, y_sem.at[zz, p])

    def to_core(zz, yy, p):
        return send(ident(zz, yy, c), p, c_peer, c_sem.at[2 * zz + yy, p])

    def to_above(zz, p):
        return send(ident(zz, y, c), p, me + 4, up_sem.at[zz, p])

    def to_below(zz, p):
        return send(ident(zz, y, c), p, me - 4, down_sem.at[zz, p])

    def publish(p):
        to_core(z, y, p).start()
        to_y(z, p).start()
        pl.when(above)(lambda: to_above(z, p).start())
        pl.when(below)(lambda: to_below(z, p).start())

    own_first, own_second = span_ref[0, me], span_ref[1, me]
    within = lax.broadcasted_iota(jnp.int32, (rows, HEAD), 0)
    position = jnp.where(
        within < half, own_first * half + within, own_second * half + within - half
    )
    angles = position.astype(F32) * inverse_ref[...]
    cosine = jnp.cos(angles)
    sine = jnp.sin(angles)
    lane = lax.broadcasted_iota(jnp.int32, (rows, HEAD), 1)
    sine = jnp.where(lane < HEAD // 2, -sine, sine)

    def finished(entries, gains):
        square = jnp.mean(entries * entries, axis=-1, keepdims=True)
        entries = entries * lax.rsqrt(square + EPSILON) * gains
        return (entries * cosine + pltpu.roll(entries, HEAD // 2, 1) * sine).astype(BF16)

    load_h.wait()
    hidden = hidden_ref[...].astype(F32)
    mean_square = jnp.mean(hidden * hidden, axis=-1, keepdims=True)
    normed = (hidden * lax.rsqrt(mean_square + EPSILON) * gain_ref[...]).astype(BF16)

    load_k.wait()
    load_v.wait()
    for copy in load_q:
        copy.start()
    keys = jnp.dot(normed, wk_ref[...], preferred_element_type=F32)
    for g in range(kv_heads):
        cut = slice(g * HEAD, (g + 1) * HEAD)
        kv_ref[me, 0, :, cut] = finished(keys[:, cut], kgain_ref[...])
    pl.semaphore_wait(barrier, 2 + jnp.where(below, 1, 0) + jnp.where(above, 1, 0))
    publish(0)
    kv_ref[me, 1] = jnp.dot(normed, wv_ref[...], preferred_element_type=F32).astype(BF16)
    publish(1)

    ordered = own_first < own_second
    own_low = jnp.minimum(own_first, own_second)
    def query(i):
        load_q[i].wait()
        part = jnp.dot(normed, wq_ref[i], preferred_element_type=F32)
        for j in range(chunk // HEAD):
            head = i * (chunk // HEAD) + j
            done = finished(part[:, j * HEAD:(j + 1) * HEAD], qgain_ref[...])
            g, r = head // group, head % group
            first, second = done[:half], done[half:]
            q_ref[g, r * half:(r + 1) * half, :HEAD] = jnp.where(ordered, first, second)
            q_ref[g, r * half:(r + 1) * half, HEAD:] = jnp.where(ordered, second, first)

    def transposed_dot(a, b):
        return lax.dot_general(a, b, (((1,), (1,)), ((), ())), preferred_element_type=F32)

    def block_peak(block):
        tall = block.shape[0]
        return jnp.max(block.reshape(tall // 8, 8, wide), axis=0)

    visible = (
        lax.broadcasted_iota(jnp.int32, (half, wide), 0)
        <= lax.broadcasted_iota(jnp.int32, (half, wide), 1) % half
    )

    def score(zz, k, own, peaks):
        sources = []
        for yy, cc in ((y, c), (y, 1 - c), (1 - y, c), (1 - y, 1 - c)):
            src = ident(zz, yy, cc)
            upper = span_ref[0, src] > span_ref[1, src]
            early = jnp.minimum(span_ref[0, src], span_ref[1, src]) < own_low
            sources.append((src, upper, early))
        for g in range(kv_heads):
            cut = slice(g * HEAD, (g + 1) * HEAD)

            def piece(src, part, upper):
                first = kv_ref[src, part, :half, cut]
                second = kv_ref[src, part, half:, cut]
                return jnp.where(upper, second, first)

            span = slice(k * 4 * half, (k + 1) * 4 * half)
            low_keys = jnp.concatenate([piece(s, 0, up) for s, up, e in sources], axis=0)
            scores = transposed_dot(low_keys, q_ref[g, :, HEAD:])
            s_ref[g, 0, span, :] = scores
            peaks[g][1] = jnp.maximum(peaks[g][1], block_peak(scores))
            low_values = jnp.concatenate([piece(s, 1, up) for s, up, e in sources], axis=0)
            vta_ref[g, :, span] = low_values.T

            def parted(part):
                early_side, late_side = [], []
                for src, upper, early in sources:
                    block = piece(src, part, upper == early)
                    early_side.append(jnp.where(early, block, jnp.zeros_like(block)))
                    late_side.append(jnp.where(early, jnp.zeros_like(block), block))
                return jnp.concatenate(
                    [jnp.concatenate(early_side, axis=0), jnp.concatenate(late_side, axis=0)],
                    axis=1,
                )

            mixed = transposed_dot(parted(0), q_ref[g])
            for j, (src, upper, early) in enumerate(sources):
                scores = mixed[j * half:(j + 1) * half]
                if own and j == 0:
                    scores = jnp.where(visible, scores, LOW)
                at = (k * 4 + j) * half
                s_ref[g, 1, at:at + half, :] = scores
                peak = block_peak(scores)
                peaks[g][0] = jnp.maximum(peaks[g][0], jnp.where(early, peak, LOW))
                peaks[g][1] = jnp.maximum(peaks[g][1], jnp.where(early, LOW, peak))
            vtb_ref[g, :, span] = parted(1).T
            if own:
                src, upper, early = sources[0]
                scores = transposed_dot(piece(src, 0, upper), q_ref[g, :, :HEAD])
                scores = jnp.where(visible, scores, LOW)
                s_ref[g, 1, 16 * half:17 * half, :] = scores
                peaks[g][0] = jnp.maximum(peaks[g][0], block_peak(scores))
                vtc_ref[g] = piece(src, 1, upper).T

    def forward(t, p):
        def from_below():
            arrived(me - 4 * t, p)
            pl.when(above)(lambda: to_above(z - t, p).start())
            to_y(z - t, p).start()
            to_core(z - t, y, p).start()

        def from_above():
            arrived(me + 4 * t, p)
            pl.when(below)(lambda: to_below(z + t, p).start())
            to_y(z + t, p).start()
            to_core(z + t, y, p).start()

        pl.when(z >= t)(from_below)
        pl.when(z + t < lanes_z)(from_above)

    def pass_on(zz, p):
        arrived(ident(zz, 1 - y, c), p)
        to_core(zz, 1 - y, p).start()

    def last(zz):
        for p in range(2):
            arrived(ident(zz, y, 1 - c), p)
            arrived(ident(zz, 1 - y, 1 - c), p)

    def sums(block):
        tall = block.shape[0]
        return jnp.sum(block.reshape(tall // 8, 8, wide), axis=0)

    def absorb(g, step, parts, first, peaks):
        span = slice(parts[0] * 4 * half, (parts[-1] + 1) * 4 * half)
        if True:
            new = [jnp.max(peaks[g][t], axis=0, keepdims=True) for t in range(2)]
            if not first:
                new = [jnp.maximum(new[t], peak_ref[g, t]) for t in range(2)]
            totals = [jnp.zeros((8, wide), F32), jnp.zeros((8, wide), F32)]
            for k in parts:
                at = k * 4 * half
                weight = jnp.exp2((s_ref[g, 0, at:at + 4 * half, :] - new[1]) * FACTOR)
                totals[1] = totals[1] + sums(weight)
                pa_ref[at:at + 4 * half, :] = weight.astype(BF16)
                for j, (yy, cc) in enumerate(
                    ((y, c), (y, 1 - c), (1 - y, c), (1 - y, 1 - c))
                ):
                    src = ident(place(step, k), yy, cc)
                    early = jnp.minimum(span_ref[0, src], span_ref[1, src]) < own_low
                    spot = at + j * half
                    peak = jnp.where(early, new[0], new[1])
                    weight = jnp.exp2((s_ref[g, 1, spot:spot + half, :] - peak) * FACTOR)
                    part = sums(weight)
                    totals[0] = totals[0] + jnp.where(early, part, 0.0)
                    totals[1] = totals[1] + jnp.where(early, 0.0, part)
                    pb_ref[spot:spot + half, :] = weight.astype(BF16)
            mixed = jnp.dot(
                vtb_ref[g, :, span], pb_ref[span, :], preferred_element_type=F32
            )
            added = [
                mixed[:HEAD],
                mixed[HEAD:] + jnp.dot(
                    vta_ref[g, :, span], pa_ref[span, :], preferred_element_type=F32
                ),
            ]
            if first:
                weight = jnp.exp2((s_ref[g, 1, 16 * half:17 * half, :] - new[0]) * FACTOR)
                totals[0] = totals[0] + sums(weight)
                added[0] = added[0] + jnp.dot(
                    vtc_ref[g], weight.astype(BF16), preferred_element_type=F32
                )
            for t in range(2):
                total = jnp.sum(totals[t], axis=0, keepdims=True)
                if first:
                    acc_ref[g, t] = added[t]
                    total_ref[g, t] = total
                else:
                    decay = jnp.exp2((peak_ref[g, t] - new[t]) * FACTOR)
                    acc_ref[g, t] = acc_ref[g, t] * decay + added[t]
                    total_ref[g, t] = total_ref[g, t] * decay + total
                peak_ref[g, t] = new[t]

    def nothing():
        return [[jnp.full((8, wide), LOW, F32) for t in range(2)] for g in range(kv_heads)]

    everything = range(4)
    peaks = nothing()
    if lanes_z == 4:
        z1, z2, z3 = (place(0, k) for k in range(1, 4))
        for i in range(chunks // 2):
            query(i)
        forward(1, 0)
        pass_on(z, 0)
        for i in range(chunks // 2, chunks - 1):
            query(i)
        forward(1, 1)
        pass_on(z, 1)
        query(chunks - 1)
        forward(2, 0)
        pass_on(z1, 0)
        last(z)
        score(z, 0, True, peaks)
        forward(2, 1)
        pass_on(z1, 1)
        last(z1)
        score(z1, 1, False, peaks)
        forward(3, 0)
        pass_on(z2, 0)
        absorb(0, 0, (0, 1), True, peaks)
        forward(3, 1)
        pass_on(z2, 1)
        for g in range(1, kv_heads):
            absorb(g, 0, (0, 1), True, peaks)
        pass_on(z3, 0)
        peaks = nothing()
        last(z2)
        score(z2, 2, False, peaks)
        pass_on(z3, 1)
        last(z3)
        score(z3, 3, False, peaks)
        for g in range(kv_heads):
            absorb(g, 0, (2, 3), False, peaks)
    else:
        for i in range(chunks):
            query(i)
        for p in range(2):
            pass_on(z, p)

        def relay(t, carry):
            for p in range(2):
                forward(t, p)
                pl.when(z >= t)(lambda: pass_on(z - t, p))
                pl.when(z + t < lanes_z)(lambda: pass_on(z + t, p))
            return carry

        lax.fori_loop(1, lanes_z, relay, 0)
        last(z)
        score(z, 0, True, peaks)
        for k in range(1, 4):
            last(place(0, k))
            score(place(0, k), k, False, peaks)
        for g in range(kv_heads):
            absorb(g, 0, everything, True, peaks)

        def further(step, carry):
            peaks = nothing()
            for k in everything:
                last(place(step, k))
                score(place(step, k), k, False, peaks)
            for g in range(kv_heads):
                absorb(g, step, everything, False, peaks)
            return carry

        lax.fori_loop(1, lanes_z // 4, further, 0)

    for g in range(kv_heads):
        low = acc_ref[g, 0] / total_ref[g, 0]
        high = acc_ref[g, 1] / total_ref[g, 1]
        for r in range(0, group, 2):
            low_rows = low[:, r * half:(r + 2) * half].T
            high_rows = high[:, r * half:(r + 2) * half].T
            first = jnp.where(ordered, low_rows, high_rows).astype(BF16)
            second = jnp.where(ordered, high_rows, low_rows).astype(BF16)
            for e in range(2):
                at = (g * group + r + e) * HEAD
                out_ref[:half, at:at + HEAD] = first[e * half:(e + 1) * half]
                out_ref[half:, at:at + HEAD] = second[e * half:(e + 1) * half]

    def drain(zz, carry):
        for p in range(2):
            to_y(zz, p).wait_send()
            to_core(zz, 0, p).wait_send()
            to_core(zz, 1, p).wait_send()
            pl.when(jnp.logical_and(zz <= z, above))(lambda: to_above(zz, p).wait_send())
            pl.when(jnp.logical_and(zz >= z, below))(lambda: to_below(zz, p).wait_send())
        return carry

    lax.fori_loop(0, lanes_z, drain, 0)


def solution(mesh):
    n = mesh.shape["ctx"]

    def body(hidden_in, span_order, norm_gain, w_query, w_key, w_value, query_gain, key_gain):
        rows, depth = hidden_in.shape
        heads, kv_heads = w_query.shape[1] // HEAD, w_key.shape[1] // HEAD
        half = rows // 2
        wide = heads // kv_heads * half
        frequency = THETA ** (-np.arange(HEAD // 2, dtype=np.float64) * (2.0 / HEAD))
        inverse = jnp.asarray(np.tile(frequency, 2)[None, :], F32)
        vmem = pl.BlockSpec(memory_space=pltpu.VMEM)
        anywhere = pl.BlockSpec(memory_space=pl.ANY)
        chunk = 4 * HEAD
        chunks = heads * HEAD // chunk
        return pl.pallas_call(
            functools.partial(kernel, n, heads, kv_heads),
            out_shape=jax.ShapeDtypeStruct((rows, heads * HEAD), BF16),
            in_specs=[
                anywhere, pl.BlockSpec(memory_space=pltpu.SMEM), vmem,
                anywhere, anywhere, anywhere, vmem, vmem, vmem,
            ],
            out_specs=vmem,
            scratch_shapes=[
                pltpu.VMEM((rows, depth), BF16),
                pltpu.VMEM((chunks, depth, chunk), BF16),
                pltpu.VMEM((depth, kv_heads * HEAD), BF16),
                pltpu.VMEM((depth, kv_heads * HEAD), BF16),
                pltpu.VMEM((n, 2, rows, kv_heads * HEAD), BF16),
                pltpu.VMEM((kv_heads, wide, 2 * HEAD), BF16),
                pltpu.VMEM((kv_heads, 2, 17 * half, wide), F32),
                pltpu.VMEM((kv_heads, HEAD, 16 * half), BF16),
                pltpu.VMEM((kv_heads, 2 * HEAD, 16 * half), BF16),
                pltpu.VMEM((kv_heads, HEAD, half), BF16),
                pltpu.VMEM((16 * half, wide), BF16),
                pltpu.VMEM((16 * half, wide), BF16),
                pltpu.VMEM((kv_heads, 2, HEAD, wide), F32),
                pltpu.VMEM((kv_heads, 2, 1, wide), F32),
                pltpu.VMEM((kv_heads, 2, 1, wide), F32),
                pltpu.SemaphoreType.DMA((3 + chunks,)),
                pltpu.SemaphoreType.DMA((n, 2)),
                pltpu.SemaphoreType.DMA((n // 4, 2)),
                pltpu.SemaphoreType.DMA((n // 4, 2)),
                pltpu.SemaphoreType.DMA((n // 4, 2)),
                pltpu.SemaphoreType.DMA((n // 2, 2)),
            ],
            compiler_params=pltpu.CompilerParams(
                collective_id=0, has_side_effects=True, vmem_limit_bytes=60 * 1024 * 1024
            ),
        )(
            hidden_in, span_order.T, norm_gain.reshape(1, -1), w_query, w_key, w_value,
            query_gain.reshape(1, -1), key_gain.reshape(1, -1), inverse,
        )

    in_specs = (P(("groups", "ctx"), None), P("groups", None), P(), P(), P(), P(), P(), P())
    out_specs = P(("groups", "ctx"), None)
    return jax.shard_map(body, mesh=mesh, in_specs=in_specs, out_specs=out_specs, check_vma=False)
```
